32 devices in a mesh: gx: 8 (over z, core), gz: 4 (over y, x).
Axes of the slice: x: 2, y: 2, z: 4, core: 2. Of those that a mesh axis runs over, the one named last changes fastest.
Arguments:
- view_index: int32 [1], replicated, may hold values from 0 to 5
- psf_taps: float32 [6, 3, 31], replicated, may hold values from 0.1 to 1
- extents: int32 [6, 3], replicated, may hold values from 4 to 15
- estimate: float32 [16, 256, 1024], P(None, 'gz', 'gx'), may hold values from 0.5 to 2
- measured: float32 [16, 256, 1024], P(None, 'gz', 'gx'), may hold values from 0.25 to 4
Outputs:
- upsampled: float32 [16, 1024, 1024], P('gz', None, 'gx')
The draws below stay inside these ranges and needn't reach their ends.
All inputs are finite; a program needn't handle non-finite values.
Results may differ from the reference program's by a relative error of at most 0.004.
Values may be sent and summed in bfloat16 or wider, within the bound.
A program may use at most 64 MiB of HBM per device.

```python
import math
import jax
import jax.numpy as jnp
from jax import lax

Y = 16
HALF = 15
TAPS = 31
VIEWS = 6
UP = 4
NX = 1024
NZ = 256


def with_ends(result, own_key, low, largest):
    spot = [jax.random.randint(jax.random.fold_in(own_key, axis), (), 0, length) for axis, length in enumerate(result.shape)]
    widest = result.shape.index(max(result.shape))
    next_to = spot[:widest] + [(spot[widest] + 1) % result.shape[widest]] + spot[widest + 1:]
    return result.at[tuple(spot)].set(low).at[tuple(next_to)].set(largest)


def block_levels(stream_key, dims, split, low, top_value):
    loudness, own = 1.0, jax.random.fold_in(stream_key, 6)
    for dim, blocks in split:
        steps = jnp.exp(jax.random.uniform(jax.random.fold_in(own, dim), (blocks,), jnp.float32, low / len(split), top_value / len(split)))
        loudness = loudness * jnp.repeat(steps, dims[dim] // blocks).reshape([-1 if axis == dim else 1 for axis in range(len(dims))])
    return loudness


def setup_inputs(seed: int = 0) -> dict:
    seeds = jax.random.split(jax.random.key(seed), 6)
    return {
        "view_index": jax.random.randint(seeds[0], (1,), 0, VIEWS).astype(jnp.int32),
        "psf_taps": jnp.clip(jnp.exp(jax.random.uniform(seeds[1], (VIEWS, 3, TAPS), jnp.float32, math.log(0.1), math.log(1.0))), 0.1, 1.0),
        "extents": with_ends(jax.random.randint(seeds[2], (VIEWS, 3), 4, HALF + 1), jax.random.fold_in(seeds[2], 1), 4, HALF).astype(jnp.int32),
        "estimate": jnp.clip(jnp.exp(math.log(2.0) - 1.3862944 * jax.random.uniform(seeds[3], (Y, NZ, NX), jnp.float32) ** block_levels(seeds[3], (Y, NZ, NX), ((1, 4), (2, 8)), -0.2, 0.2)), 0.5, 2.0),
        "measured": jnp.clip(jnp.exp(math.log(4.0) - 2.7725887 * jax.random.uniform(seeds[4], (Y, NZ, NX), jnp.float32) ** block_levels(seeds[4], (Y, NZ, NX), ((1, 4), (2, 8)), -0.2, 0.2)), 0.25, 4.0),
    }


def pick_kernels(view_index, psf_taps, extents):
    chosen = view_index[0]
    offsets = jnp.arange(TAPS, dtype=jnp.int32) - HALF
    kernels = []
    for axis_id in range(3):
        unnormalized_taps = psf_taps[chosen, axis_id] * (jnp.abs(offsets) <= extents[chosen, axis_id]).astype(jnp.float32)
        kernels.append(unnormalized_taps / jnp.sum(unnormalized_taps))
    return kernels


def smear(volume, kernel, axis_dim):
    length = volume.shape[axis_dim]
    pad_widths = [(0, 0), (0, 0), (0, 0)]
    pad_widths[axis_dim] = (HALF, HALF)
    padded = jnp.pad(volume, pad_widths)
    total = jnp.zeros_like(volume)
    for tap_index in range(TAPS):
        total = total + kernel[tap_index] * lax.slice_in_dim(padded, tap_index, tap_index + length, axis=axis_dim)
    return total


def blur(volume, kernels):
    section_one = smear(volume, kernels[0], 2)
    section_two = smear(section_one, kernels[1], 0)
    return smear(section_two, kernels[2], 1)


def build_table(first_row, count_of_rows, length):
    row_ids = first_row + jnp.arange(count_of_rows, dtype=jnp.int32)[:, None]
    column_numbers = jnp.arange(length, dtype=jnp.int32)[None, :]
    offset_units = jnp.mod(row_ids - UP * column_numbers, UP * length)
    sine_part = jnp.sin(jnp.pi * jnp.mod(offset_units, 2 * UP).astype(jnp.float32) / UP)
    tangent_part = length * jnp.tan(jnp.pi * offset_units.astype(jnp.float32) / (UP * length))
    on_grid = jnp.mod(offset_units, UP) == 0
    guarded_denominator = jnp.where(on_grid, jnp.float32(1.0), tangent_part)
    entries = jnp.where(on_grid, jnp.where(offset_units == 0, jnp.float32(1.0), jnp.float32(0.0)), sine_part / guarded_denominator)
    return entries.astype(jnp.bfloat16)


def reference(view_index, psf_taps, extents, estimate, measured):
    kernels = pick_kernels(view_index, psf_taps, extents)
    blurred = blur(estimate, kernels)
    quotient = measured / blurred
    correction = blur(quotient, [kernel[::-1] for kernel in kernels])
    rounded = (estimate * correction).astype(jnp.bfloat16)
    full_table = build_table(0, UP * NZ, NZ)

    def per_plane(slab_plane):
        return jnp.dot(full_table, slab_plane, preferred_element_type=jnp.float32)

    return lax.map(per_plane, rounded)
```

```python
import functools

import jax
import jax.numpy as jnp
from jax import lax
from jax.experimental import pallas as pl
from jax.experimental.pallas import tpu as pltpu
from jax.sharding import PartitionSpec as P

HALF = 15
TAPS = 31
UP = 4
PAD = 16
BF = jnp.bfloat16
F32 = jnp.float32
MESH = pl.DeviceIdType.MESH
AROUND = [(dx, dz) for dz in (-1, 1, 0) for dx in (0, -1, 1) if (dx, dz) != (0, 0)]


def dot(a, b):
    return jnp.dot(a, b, preferred_element_type=F32)


def lanes_of(shape):
    return lax.broadcasted_iota(jnp.int32, shape, 1)


def rows_of(shape):
    return lax.broadcasted_iota(jnp.int32, shape, 0)


def tap_row(taps_ref, view, extents_ref, axis_id, width, spread, flip):
    lane = lanes_of((8, width))
    row = jnp.zeros((8, width), F32)
    for t in range(TAPS):
        spot = (TAPS - 1 - t if flip else t) * spread
        row = jnp.where(lane == spot, taps_ref[view, axis_id, t], row)
    keep = jnp.abs(lane - HALF * spread) <= extents_ref[view, axis_id] * spread
    row = jnp.where(keep, row, 0.0)
    return row / jnp.sum(row, axis=1, keepdims=True)


def slanted(row, count, shift):
    width = row.shape[1]
    tall = jnp.broadcast_to(row[0:1], (count, width))
    return pltpu.roll(tall, shift % width, 1, stride=1, stride_axis=0)


def make_matrices(taps_ref, view, extents_ref, flip, mz, too, wide, ky, ny, nz, nx):
    group = nx // PAD
    mz[...] = slanted(tap_row(taps_ref, view, extents_ref, 2, nx, 1, flip), nz, 1)[
        :, : nz + 2 * PAD
    ].astype(BF)
    ring = slanted(tap_row(taps_ref, view, extents_ref, 0, nx, 1, not flip), nx, -HALF)
    lane, row = lanes_of((nx, nx)), rows_of((nx, nx))
    too[...] = jnp.where(jnp.abs(lane - row) <= HALF, ring, 0.0).astype(BF)
    edge = lanes_of((PAD, nx))
    from_left = jnp.where(edge < nx // 2, ring[nx - PAD :], 0.0).astype(BF)
    from_right = jnp.where(edge >= nx // 2, ring[:PAD], 0.0).astype(BF)
    wide[...] = jnp.zeros(wide.shape, BF)
    for j in range(group):
        wide[j * PAD : (j + 1) * PAD, j * nx : (j + 1) * nx] = from_left
        wide[nx + j * PAD : nx + (j + 1) * PAD, j * nx : (j + 1) * nx] = from_right
    sub = 8
    long = tap_row(taps_ref, view, extents_ref, 1, 2 * ny * sub, sub, flip)
    ky[...] = slanted(long, ny * sub, -HALF * sub)[:, : ny * sub].astype(BF)


def make_table(table, length):
    shape = (PAD, length)
    offset = jnp.bitwise_and(rows_of(shape) - UP * lanes_of(shape), UP * length - 1)
    sine = jnp.sin(jnp.pi * jnp.bitwise_and(offset, 2 * UP - 1).astype(F32) / UP)
    angle = jnp.pi * offset.astype(F32) / (UP * length)
    on_grid = jnp.bitwise_and(offset, UP - 1) == 0
    below = jnp.where(on_grid, 1.0, length * jnp.sin(angle) / jnp.where(on_grid, 1.0, jnp.cos(angle)))
    first = jnp.where(on_grid, jnp.where(offset == 0, 1.0, 0.0), sine / below)

    def fill(j, carry):
        table[pl.ds(pl.multiple_of(j * PAD, PAD), PAD), :] = pltpu.roll(
            first, j * (PAD // UP), 1
        ).astype(BF)
        return carry

    lax.fori_loop(0, UP * length // PAD, fill, 0)


def pack_edges(volume, packed, ny, nz, nx):
    group = nx // PAD
    lane = lanes_of((nz, nx)) // PAD
    for g in range(ny // group):
        left = right = None
        for j in range(group):
            plane = volume(g * group + j)
            a = pltpu.roll(plane, (j * PAD) % nx, 1) if j else plane
            s = (j * PAD - (nx - PAD)) % nx
            b = pltpu.roll(plane, s, 1) if s else plane
            left = a if left is None else jnp.where(lane == j, a, left)
            right = b if right is None else jnp.where(lane == j, b, right)
        packed[0, g] = left.astype(BF)
        packed[1, g] = right.astype(BF)


def blur(ext, side, mz, too, wide, ky, held, ny, nz, nx):
    group = nx // PAD
    m = mz[...]
    s = [
        jnp.concatenate([dot(m, side[q, g]) for q in range(2)], axis=1).astype(BF)
        for g in range(ny // group)
    ]
    vs = [dot(part, wide[...]) for part in s]
    for y in range(ny):
        u = dot(m, ext[y]).astype(BF)
        g, j = divmod(y, group)
        held[y] = dot(u, too[...]) + vs[g][:, j * nx : (j + 1) * nx]
    for k in range(nz // 8):
        a = held[:, k * 8 : (k + 1) * 8, :].reshape(ny * 8, nx).astype(BF)
        yield k, dot(ky[...], a).reshape(ny, 8, nx)


def kernel(
    ngx, ngz,
    view_ref, taps_ref, extents_ref, est_ref, mea_ref,
    out_ref, table_ref,
    ext, side, packed, gathered, leaving, held, quot,
    mz, too, wide, ky,
    send_sem, recv_sem, all_send, all_recv,
):
    ny, nz, nx = est_ref.shape
    planes = ny // ngz
    gx, gz = lax.axis_index("gx"), lax.axis_index("gz")
    has_x = {-1: gx > 0, 0: True, 1: gx < ngx - 1}
    has_z = {-1: gz > 0, 0: True, 1: gz < ngz - 1}

    def there(dx, dz):
        if dx == 0:
            return has_z[dz]
        if dz == 0:
            return has_x[dx]
        return jnp.logical_and(has_x[dx], has_z[dz])

    barrier = pltpu.get_barrier_semaphore()
    total = ngz - 1
    for d in range(1, ngz):
        pl.semaphore_signal(
            barrier, inc=1, device_id=(gx, lax.rem(gz + d, ngz)), device_id_type=MESH
        )
    for dx, dz in AROUND:
        if dx == 0:
            continue
        here = there(dx, dz)
        total = total + jnp.where(here, 1, 0)

        @pl.when(here)
        def _(dx=dx, dz=dz):
            pl.semaphore_signal(
                barrier, inc=1, device_id=(gx + dx, gz + dz), device_id_type=MESH
            )

    def landing(r, dx, dz):
        first, count = {-1: (0, PAD), 0: (PAD, nz), 1: (PAD + nz, PAD)}[dz]
        rows = pl.ds(first, count)
        if dx == 0:
            return ext.at[r, :, rows, :]
        return side.at[r, 0 if dx < 0 else 1, :, rows, :]

    def copy(r, dx, dz):
        first, count = {-1: (0, PAD), 0: (0, nz), 1: (nz - PAD, PAD)}[dz]
        if dx == 0:
            src = ext.at[r, :, pl.ds(PAD + first, count), :]
        else:
            src = packed.at[r, 0 if dx < 0 else 1, :, pl.ds(first, count), :]
        return pltpu.make_async_remote_copy(
            src_ref=src,
            dst_ref=landing(r, -dx, -dz),
            send_sem=send_sem.at[r, AROUND.index((dx, dz))],
            recv_sem=recv_sem.at[r, AROUND.index((-dx, -dz))],
            device_id=(gx + dx, gz + dz),
            device_id_type=MESH,
        )

    def arrival(r, dx, dz):
        first, count = {-1: (0, PAD), 0: (0, nz), 1: (nz - PAD, PAD)}[dz]
        dst = landing(r, dx, dz)
        return pltpu.make_async_remote_copy(
            src_ref=dst,
            dst_ref=dst,
            send_sem=send_sem.at[r, AROUND.index((dx, dz))],
            recv_sem=recv_sem.at[r, AROUND.index((dx, dz))],
            device_id=(gx + dx, gz + dz),
            device_id_type=MESH,
        )

    def clear(r):
        for dx, dz in AROUND:
            @pl.when(jnp.logical_not(there(dx, dz)))
            def _(dx=dx, dz=dz):
                spot = landing(r, dx, dz)
                spot[...] = jnp.zeros(spot.shape, BF)

    def send(r):
        for dx, dz in AROUND:
            @pl.when(there(dx, dz))
            def _(dx=dx, dz=dz):
                copy(r, dx, dz).start()

    def receive(r):
        for dx, dz in AROUND:
            @pl.when(there(dx, dz))
            def _(dx=dx, dz=dz):
                arrival(r, dx, dz).wait_recv()

    def sent(r):
        for dx, dz in AROUND:
            @pl.when(there(dx, dz))
            def _(dx=dx, dz=dz):
                copy(r, dx, dz).wait_send()

    ext[0, :, PAD : PAD + nz, :] = est_ref[...].astype(BF)
    pack_edges(lambda y: est_ref[y], packed.at[0], ny, nz, nx)
    pl.semaphore_wait(barrier, total)
    send(0)

    view = view_ref[0]
    for flip in range(2):
        make_matrices(
            taps_ref, view, extents_ref, bool(flip),
            mz.at[flip], too.at[flip], wide.at[flip], ky.at[flip], ny, nz, nx,
        )
    clear(0)
    clear(1)
    make_table(table_ref, nz * ngz)
    receive(0)
    for k, value in blur(ext.at[0], side.at[0], mz[0], too[0], wide[0], ky[0], held, ny, nz, nx):
        rows = pl.ds(k * 8, 8)
        quot[:, rows, :] = mea_ref[:, rows, :] / value
    ext[1, :, PAD : PAD + nz, :] = quot[...].astype(BF)
    pack_edges(lambda y: quot[y], packed.at[1], ny, nz, nx)
    send(1)
    receive(1)
    for k, value in blur(ext.at[1], side.at[1], mz[1], too[1], wide[1], ky[1], held, ny, nz, nx):
        rows = pl.ds(k * 8, 8)
        quot[:, rows, :] = est_ref[:, rows, :] * value
    leaving[...] = quot[...].astype(BF)

    def exchange(d):
        to = lax.rem(gz + d, ngz)
        return pltpu.make_async_remote_copy(
            src_ref=leaving.at[pl.ds(to * planes, planes)],
            dst_ref=gathered.at[:, pl.ds(pl.multiple_of(gz * nz, nz), nz), :],
            send_sem=all_send.at[d],
            recv_sem=all_recv.at[d],
            device_id=(gx, to),
            device_id_type=MESH,
        )

    for d in range(1, ngz):
        exchange(d).start()
    mine = pl.ds(pl.multiple_of(gz * nz, nz), nz)
    gathered[:, mine, :] = leaving[pl.ds(gz * planes, planes)]
    for d in range(1, ngz):
        exchange(d).wait_recv()
    out_ref[...] = gathered[...]
    sent(0)
    sent(1)
    for d in range(1, ngz):
        exchange(d).wait_send()


def upsample_kernel(table_ref, lines_ref, out_ref):
    out_ref[0] = dot(table_ref[...], lines_ref[0])


def on_device(ngx, ngz, view_index, psf_taps, extents, estimate, measured):
    ny, nz, nx = estimate.shape
    planes, lines = ny // ngz, nz * ngz
    group = nx // PAD
    smem = pl.BlockSpec(memory_space=pltpu.SMEM)
    vmem = pl.BlockSpec(memory_space=pltpu.VMEM)
    gathered, table = pl.pallas_call(
        functools.partial(kernel, ngx, ngz),
        out_shape=[
            jax.ShapeDtypeStruct((planes, lines, nx), BF),
            jax.ShapeDtypeStruct((UP * lines, lines), BF),
        ],
        in_specs=[smem, smem, smem, vmem, vmem],
        out_specs=[vmem, vmem],
        scratch_shapes=[
            pltpu.VMEM((2, ny, nz + 2 * PAD, nx), BF),
            pltpu.VMEM((2, 2, ny // group, nz + 2 * PAD, nx), BF),
            pltpu.VMEM((2, 2, ny // group, nz, nx), BF),
            pltpu.VMEM((planes, lines, nx), BF),
            pltpu.VMEM((ny, nz, nx), BF),
            pltpu.VMEM((ny, nz, nx), F32),
            pltpu.VMEM((ny, nz, nx), F32),
            pltpu.VMEM((2, nz, nz + 2 * PAD), BF),
            pltpu.VMEM((2, nx, nx), BF),
            pltpu.VMEM((2, 2 * nx, group * nx), BF),
            pltpu.VMEM((2, ny * 8, ny * 8), BF),
            pltpu.SemaphoreType.DMA((2, 8)),
            pltpu.SemaphoreType.DMA((2, 8)),
            pltpu.SemaphoreType.DMA((ngz,)),
            pltpu.SemaphoreType.DMA((ngz,)),
        ],
        compiler_params=pltpu.CompilerParams(collective_id=0, has_side_effects=True),
    )(view_index, psf_taps, extents, estimate, measured)
    return pl.pallas_call(
        upsample_kernel,
        grid=(planes,),
        out_shape=jax.ShapeDtypeStruct((planes, UP * lines, nx), F32),
        in_specs=[
            pl.BlockSpec((UP * lines, lines), lambda y: (0, 0)),
            pl.BlockSpec((1, lines, nx), lambda y: (y, 0, 0)),
        ],
        out_specs=pl.BlockSpec((1, UP * lines, nx), lambda y: (y, 0, 0)),
    )(table, gathered)


def solution(mesh):
    return jax.shard_map(
        functools.partial(on_device, mesh.shape["gx"], mesh.shape["gz"]),
        mesh=mesh,
        in_specs=(P(), P(), P(), P(None, "gz", "gx"), P(None, "gz", "gx")),
        out_specs=P("gz", None, "gx"),
        check_vma=False,
    )
```

```python
import functools

import jax
import jax.numpy as jnp
from jax import lax
from jax.experimental import pallas as pl
from jax.experimental.pallas import tpu as pltpu
from jax.sharding import PartitionSpec as P

HALF = 15
TAPS = 31
UP = 4
PAD = 16
BF = jnp.bfloat16
F32 = jnp.float32
MESH = pl.DeviceIdType.MESH
AROUND = [(dx, dz) for dz in (-1, 1, 0) for dx in (0, -1, 1) if (dx, dz) != (0, 0)]


def dot(a, b):
    return jnp.dot(a, b, preferred_element_type=F32)


def lanes_of(shape):
    return lax.broadcasted_iota(jnp.int32, shape, 1)


def rows_of(shape):
    return lax.broadcasted_iota(jnp.int32, shape, 0)


def tap_row(taps_ref, view, extents_ref, axis_id, width, spread, flip):
    lane = lanes_of((8, width))
    row = jnp.zeros((8, width), F32)
    for t in range(TAPS):
        spot = (TAPS - 1 - t if flip else t) * spread
        row = jnp.where(lane == spot, taps_ref[view, axis_id, t], row)
    keep = jnp.abs(lane - HALF * spread) <= extents_ref[axis_id, view] * spread
    row = jnp.where(keep, row, 0.0)
    return row / jnp.sum(row, axis=1, keepdims=True)


def slanted(row, count, shift):
    width = row.shape[1]
    tall = jnp.broadcast_to(row[0:1], (count, width))
    return pltpu.roll(tall, shift % width, 1, stride=1, stride_axis=0)


def make_matrices(taps_ref, view, extents_ref, flip, mz, too, wide, ky, ny, nz, nx):
    group = nx // PAD
    mz[...] = slanted(tap_row(taps_ref, view, extents_ref, 2, nx, 1, flip), nz, 1)[
        :, : nz + 2 * PAD
    ].astype(BF)
    ring = slanted(tap_row(taps_ref, view, extents_ref, 0, nx, 1, not flip), nx, -HALF)
    lane, row = lanes_of((nx, nx)), rows_of((nx, nx))
    too[...] = jnp.where(jnp.abs(lane - row) <= HALF, ring, 0.0).astype(BF)
    edge = lanes_of((PAD, nx))
    from_left = jnp.where(edge < nx // 2, ring[nx - PAD :], 0.0).astype(BF)
    from_right = jnp.where(edge >= nx // 2, ring[:PAD], 0.0).astype(BF)
    wide[...] = jnp.zeros(wide.shape, BF)
    for j in range(group):
        wide[j * PAD : (j + 1) * PAD, j * nx : (j + 1) * nx] = from_left
        wide[nx + j * PAD : nx + (j + 1) * PAD, j * nx : (j + 1) * nx] = from_right
    sub = 8
    long = tap_row(taps_ref, view, extents_ref, 1, 2 * ny * sub, sub, flip)
    ky[...] = slanted(long, ny * sub, -HALF * sub)[:, : ny * sub].astype(BF)


def make_table(table, length):
    shape = (PAD, length)
    offset = jnp.bitwise_and(rows_of(shape) - UP * lanes_of(shape), UP * length - 1)
    sine = jnp.sin(jnp.pi * jnp.bitwise_and(offset, 2 * UP - 1).astype(F32) / UP)
    angle = jnp.pi * offset.astype(F32) / (UP * length)
    on_grid = jnp.bitwise_and(offset, UP - 1) == 0
    below = jnp.where(on_grid, 1.0, length * jnp.sin(angle) / jnp.where(on_grid, 1.0, jnp.cos(angle)))
    first = jnp.where(on_grid, jnp.where(offset == 0, 1.0, 0.0), sine / below)

    for j in range(UP * length // PAD):
        moved = pltpu.roll(first, j * (PAD // UP), 1) if j else first
        table[j * PAD : (j + 1) * PAD, :] = moved.astype(BF)


def pack_edges(volume, packed, ny, nz, nx):
    group = nx // PAD
    lane = lanes_of((nz, nx)) // PAD
    for g in range(ny // group):
        left = right = None
        for j in range(group):
            plane = volume(g * group + j)
            a = pltpu.roll(plane, (j * PAD) % nx, 1) if j else plane
            s = (j * PAD - (nx - PAD)) % nx
            b = pltpu.roll(plane, s, 1) if s else plane
            left = a if left is None else jnp.where(lane == j, a, left)
            right = b if right is None else jnp.where(lane == j, b, right)
        packed[0, g] = left.astype(BF)
        packed[1, g] = right.astype(BF)


def blur_rows(start, count, ext, side, mz, too, wide, ky, held, ny, nx):
    group = nx // PAD
    reach = count + 2 * PAD
    m = mz[0:count, 0:reach]
    near = pl.ds(start, reach)
    s = [
        jnp.concatenate([dot(m, side[q, g, near, :]) for q in range(2)], axis=1).astype(BF)
        for g in range(ny // group)
    ]
    vs = [dot(part, wide[...]) for part in s]
    for y in range(ny):
        u = dot(m, ext[y, near, :]).astype(BF)
        g, j = divmod(y, group)
        held[y, pl.ds(start, count), :] = dot(u, too[...]) + vs[g][:, j * nx : (j + 1) * nx]
    for k in range(start // 8, (start + count) // 8):
        a = held[:, k * 8 : (k + 1) * 8, :].reshape(ny * 8, nx).astype(BF)
        yield pl.ds(k * 8, 8), dot(ky[...], a).reshape(ny, 8, nx)


def kernel(
    ngx, ngz,
    view_ref, taps_ref, extents_ref, est_hbm, mea_hbm,
    out_ref,
    est_ref, mea_ref, table_ref,
    ext, side, packed, gathered, leaving, held, quot,
    mz, too, wide, ky,
    send_sem, recv_sem, all_send, all_recv, load_sem,
):
    load_est = pltpu.make_async_copy(est_hbm, est_ref, load_sem.at[0])
    load_mea = pltpu.make_async_copy(mea_hbm, mea_ref, load_sem.at[1])
    load_est.start()
    load_mea.start()
    ny, nz, nx = est_ref.shape
    planes = ny // ngz
    gx, gz = lax.axis_index("gx"), lax.axis_index("gz")
    has_x = {-1: gx > 0, 0: True, 1: gx < ngx - 1}
    has_z = {-1: gz > 0, 0: True, 1: gz < ngz - 1}

    def there(dx, dz):
        if dx == 0:
            return has_z[dz]
        if dz == 0:
            return has_x[dx]
        return jnp.logical_and(has_x[dx], has_z[dz])

    barrier = pltpu.get_barrier_semaphore()
    total = ngz - 1
    for d in range(1, ngz):
        pl.semaphore_signal(
            barrier, inc=1, device_id=(gx, lax.rem(gz + d, ngz)), device_id_type=MESH
        )
    for dx, dz in AROUND:
        if dx == 0:
            continue
        here = there(dx, dz)
        total = total + jnp.where(here, 1, 0)

        @pl.when(here)
        def _(dx=dx, dz=dz):
            pl.semaphore_signal(
                barrier, inc=1, device_id=(gx + dx, gz + dz), device_id_type=MESH
            )

    def landing(r, dx, dz):
        first, count = {-1: (0, PAD), 0: (PAD, nz), 1: (PAD + nz, PAD)}[dz]
        rows = pl.ds(first, count)
        if dx == 0:
            return ext.at[r, :, rows, :]
        return side.at[r, 0 if dx < 0 else 1, :, rows, :]

    def copy(r, dx, dz):
        first, count = {-1: (0, PAD), 0: (0, nz), 1: (nz - PAD, PAD)}[dz]
        if dx == 0:
            src = ext.at[r, :, pl.ds(PAD + first, count), :]
        else:
            src = packed.at[r, 0 if dx < 0 else 1, :, pl.ds(first, count), :]
        return pltpu.make_async_remote_copy(
            src_ref=src,
            dst_ref=landing(r, -dx, -dz),
            send_sem=send_sem.at[r, AROUND.index((dx, dz))],
            recv_sem=recv_sem.at[r, AROUND.index((-dx, -dz))],
            device_id=(gx + dx, gz + dz),
            device_id_type=MESH,
        )

    def arrival(r, dx, dz):
        first, count = {-1: (0, PAD), 0: (0, nz), 1: (nz - PAD, PAD)}[dz]
        dst = landing(r, dx, dz)
        return pltpu.make_async_remote_copy(
            src_ref=dst,
            dst_ref=dst,
            send_sem=send_sem.at[r, AROUND.index((dx, dz))],
            recv_sem=recv_sem.at[r, AROUND.index((dx, dz))],
            device_id=(gx + dx, gz + dz),
            device_id_type=MESH,
        )

    def clear(r):
        for dx, dz in AROUND:
            @pl.when(jnp.logical_not(there(dx, dz)))
            def _(dx=dx, dz=dz):
                spot = landing(r, dx, dz)
                spot[...] = jnp.zeros(spot.shape, BF)

    def send(r, which):
        for dx, dz in which:
            @pl.when(there(dx, dz))
            def _(dx=dx, dz=dz):
                copy(r, dx, dz).start()

    def receive(r, which):
        for dx, dz in which:
            @pl.when(there(dx, dz))
            def _(dx=dx, dz=dz):
                arrival(r, dx, dz).wait_recv()

    def sent(r):
        for dx, dz in AROUND:
            @pl.when(there(dx, dz))
            def _(dx=dx, dz=dz):
                copy(r, dx, dz).wait_send()

    above = [(0, -1), (0, 1)]
    sideways = [(-1, 0), (1, 0)]
    corners = [d for d in AROUND if d[0] and d[1]]
    middle = [(PAD, nz - 2 * PAD)]
    ends = [(0, PAD), (nz - PAD, PAD)]
    parts = middle + ends

    def exchange(d, part):
        to = lax.rem(gz + d, ngz)
        first, count = parts[part]
        there_rows = pl.ds(pl.multiple_of(gz * nz + first, PAD), count)
        return pltpu.make_async_remote_copy(
            src_ref=leaving.at[pl.ds(to * planes, planes), pl.ds(first, count), :],
            dst_ref=gathered.at[:, there_rows, :],
            send_sem=all_send.at[d, part],
            recv_sem=all_recv.at[d, part],
            device_id=(gx, to),
            device_id_type=MESH,
        )

    def blurred(r, blocks):
        for first, count in blocks:
            yield from blur_rows(
                first, count, ext.at[r], side.at[r],
                mz.at[r], too.at[r], wide.at[r], ky.at[r], held, ny, nx,
            )

    def quotients(blocks):
        for rows, value in blurred(0, blocks):
            quot[:, rows, :] = mea_ref[:, rows, :] / value
        for first, count in blocks:
            ext[1, :, PAD + first : PAD + first + count, :] = quot[
                :, first : first + count, :
            ].astype(BF)

    def products(blocks):
        for rows, value in blurred(1, blocks):
            held[:, rows, :] = est_ref[:, rows, :] * value
        for first, count in blocks:
            rows = slice(first, first + count)
            leaving[:, rows, :] = held[:, rows, :].astype(BF)

    load_est.wait()
    ext[0, :, PAD : PAD + nz, :] = est_ref[...].astype(BF)
    pl.semaphore_wait(barrier, total)
    send(0, above)
    pack_edges(lambda y: est_ref[y], packed.at[0], ny, nz, nx)
    send(0, corners + sideways)
    view = view_ref[0]
    for flip in range(2):
        make_matrices(
            taps_ref, view, extents_ref, bool(flip),
            mz.at[flip], too.at[flip], wide.at[flip], ky.at[flip], ny, nz, nx,
        )
    clear(0)
    clear(1)
    load_mea.wait()
    receive(0, sideways)
    quotients(middle)
    receive(0, above + corners)
    quotients(ends)
    send(1, above)
    pack_edges(lambda y: quot[y], packed.at[1], ny, nz, nx)
    send(1, corners + sideways)
    make_table(table_ref, nz * ngz)
    receive(1, sideways)
    products(middle)
    for d in range(1, ngz):
        exchange(d, 0).start()
    receive(1, above + corners)
    products(ends)
    for d in range(1, ngz):
        for part in (1, 2):
            exchange(d, part).start()
    mine = pl.ds(pl.multiple_of(gz * nz, nz), nz)
    gathered[:, mine, :] = leaving[pl.ds(gz * planes, planes)]
    for d in range(1, ngz):
        for part in range(3):
            exchange(d, part).wait_recv()
    lines = jnp.concatenate([gathered[y] for y in range(planes)], axis=1)
    step = nz * ngz
    for b in range(UP):
        rows = slice(b * step, (b + 1) * step)
        whole = dot(table_ref[rows, :], lines)
        for y in range(planes):
            out_ref[y, rows, :] = whole[:, y * nx : (y + 1) * nx]
    sent(0)
    sent(1)
    for d in range(1, ngz):
        for part in range(3):
            exchange(d, part).wait_send()


def on_device(ngx, ngz, view_index, psf_taps, extents, estimate, measured):
    ny, nz, nx = estimate.shape
    planes, lines = ny // ngz, nz * ngz
    group = nx // PAD
    smem = pl.BlockSpec(memory_space=pltpu.SMEM)
    vmem = pl.BlockSpec(memory_space=pltpu.VMEM)
    anywhere = pl.BlockSpec(memory_space=pl.ANY)
    return pl.pallas_call(
        functools.partial(kernel, ngx, ngz),
        out_shape=pltpu.VMEM((planes, UP * lines, nx), F32),
        in_specs=[smem, smem, smem, anywhere, anywhere],
        out_specs=vmem,
        scratch_shapes=[
            pltpu.VMEM((ny, nz, nx), F32),
            pltpu.VMEM((ny, nz, nx), F32),
            pltpu.VMEM((UP * lines, lines), BF),
            pltpu.VMEM((2, ny, nz + 2 * PAD, nx), BF),
            pltpu.VMEM((2, 2, ny // group, nz + 2 * PAD, nx), BF),
            pltpu.VMEM((2, 2, ny // group, nz, nx), BF),
            pltpu.VMEM((planes, lines, nx), BF),
            pltpu.VMEM((ny, nz, nx), BF),
            pltpu.VMEM((ny, nz, nx), F32),
            pltpu.VMEM((ny, nz, nx), F32),
            pltpu.VMEM((2, nz, nz + 2 * PAD), BF),
            pltpu.VMEM((2, nx, nx), BF),
            pltpu.VMEM((2, 2 * nx, group * nx), BF),
            pltpu.VMEM((2, ny * 8, ny * 8), BF),
            pltpu.SemaphoreType.DMA((2, 8)),
            pltpu.SemaphoreType.DMA((2, 8)),
            pltpu.SemaphoreType.DMA((ngz, 3)),
            pltpu.SemaphoreType.DMA((ngz, 3)),
            pltpu.SemaphoreType.DMA((2,)),
        ],
        compiler_params=pltpu.CompilerParams(collective_id=0, has_side_effects=True),
    )(view_index, psf_taps, extents.T, estimate, measured)


def solution(mesh):
    return jax.shard_map(
        functools.partial(on_device, mesh.shape["gx"], mesh.shape["gz"]),
        mesh=mesh,
        in_specs=(P(), P(), P(), P(None, "gz", "gx"), P(None, "gz", "gx")),
        out_specs=P("gz", None, "gx"),
        check_vma=False,
    )
```

```python
import functools

import jax
import jax.numpy as jnp
from jax import lax
from jax.experimental import pallas as pl
from jax.experimental.pallas import tpu as pltpu
from jax.sharding import PartitionSpec as P

HALF = 15
TAPS = 31
UP = 4
PAD = 16
BF = jnp.bfloat16
F32 = jnp.float32
MESH = pl.DeviceIdType.MESH
AROUND = [(dx, dz) for dz in (-1, 1, 0) for dx in (0, -1, 1) if (dx, dz) != (0, 0)]


def dot(a, b):
    return jnp.dot(a, b, preferred_element_type=F32)


def lanes_of(shape):
    return lax.broadcasted_iota(jnp.int32, shape, 1)


def rows_of(shape):
    return lax.broadcasted_iota(jnp.int32, shape, 0)


def tap_row(taps_ref, view, extents_ref, axis_id, width, spread, flip):
    lane = lanes_of((8, width))
    row = jnp.zeros((8, width), F32)
    for t in range(TAPS):
        spot = (TAPS - 1 - t if flip else t) * spread
        row = jnp.where(lane == spot, taps_ref[view, axis_id, t], row)
    keep = jnp.abs(lane - HALF * spread) <= extents_ref[axis_id, view] * spread
    row = jnp.where(keep, row, 0.0)
    return row / jnp.sum(row, axis=1, keepdims=True)


def slanted(row, count, shift):
    width = row.shape[1]
    tall = jnp.broadcast_to(row[0:1], (count, width))
    return pltpu.roll(tall, shift % width, 1, stride=1, stride_axis=0)


def make_matrices(taps_ref, view, extents_ref, flip, mz, too, wide, ky, ny, nz, nx):
    group = nx // PAD
    mz[...] = slanted(tap_row(taps_ref, view, extents_ref, 2, nx, 1, flip), nz, 1)[
        :, : nz + 2 * PAD
    ].astype(BF)
    ring = slanted(tap_row(taps_ref, view, extents_ref, 0, nx, 1, not flip), nx, -HALF)
    lane, row = lanes_of((nx, nx)), rows_of((nx, nx))
    too[...] = jnp.where(jnp.abs(lane - row) <= HALF, ring, 0.0).astype(BF)
    edge = lanes_of((PAD, nx))
    from_left = jnp.where(edge < nx // 2, ring[nx - PAD :], 0.0).astype(BF)
    from_right = jnp.where(edge >= nx // 2, ring[:PAD], 0.0).astype(BF)
    wide[...] = jnp.zeros(wide.shape, BF)
    for j in range(group):
        wide[j * PAD : (j + 1) * PAD, j * nx : (j + 1) * nx] = from_left
        wide[nx + j * PAD : nx + (j + 1) * PAD, j * nx : (j + 1) * nx] = from_right
    sub = 8
    long = tap_row(taps_ref, view, extents_ref, 1, 2 * ny * sub, sub, flip)
    ky[...] = slanted(long, ny * sub, -HALF * sub)[:, : ny * sub].astype(BF)


def make_table(table, length):
    shape = (PAD, length)
    offset = jnp.bitwise_and(rows_of(shape) - UP * lanes_of(shape), UP * length - 1)
    sine = jnp.sin(jnp.pi * jnp.bitwise_and(offset, 2 * UP - 1).astype(F32) / UP)
    angle = jnp.pi * offset.astype(F32) / (UP * length)
    on_grid = jnp.bitwise_and(offset, UP - 1) == 0
    below = jnp.where(on_grid, 1.0, length * jnp.sin(angle) / jnp.where(on_grid, 1.0, jnp.cos(angle)))
    first = jnp.where(on_grid, jnp.where(offset == 0, 1.0, 0.0), sine / below)

    for j in range(UP * length // PAD):
        moved = pltpu.roll(first, j * (PAD // UP), 1) if j else first
        table[j * PAD : (j + 1) * PAD, :] = moved.astype(BF)


def pack_edges(volume, packed, ny, nz, nx):
    group = nx // PAD
    lane = lanes_of((nz, nx)) // PAD
    for g in range(ny // group):
        left = right = None
        for j in range(group):
            plane = volume(g * group + j)
            a = pltpu.roll(plane, (j * PAD) % nx, 1) if j else plane
            s = (j * PAD - (nx - PAD)) % nx
            b = pltpu.roll(plane, s, 1) if s else plane
            left = a if left is None else jnp.where(lane == j, a, left)
            right = b if right is None else jnp.where(lane == j, b, right)
        packed[0, g] = left.astype(BF)
        packed[1, g] = right.astype(BF)


def blur_rows(blocks, near, m, ext, side, too, wide, ky, ny, nx):
    group = nx // PAD
    lots = ny // group
    count = m.shape[0]
    lines = [ext[y, near, :] for y in range(ny)]
    lines += [side[q, g, near, :] for g in range(lots) for q in range(2)]
    along_z = dot(m, jnp.concatenate(lines, axis=1))
    own = jnp.concatenate([along_z[:, y * nx : (y + 1) * nx] for y in range(ny)], axis=0)
    rim = jnp.concatenate(
        [along_z[:, (ny + 2 * g) * nx : (ny + 2 * g + 2) * nx] for g in range(lots)], axis=0
    )
    rim = dot(rim.astype(BF), wide[...])
    rim = jnp.concatenate(
        [
            rim[g * count : (g + 1) * count, j * nx : (j + 1) * nx]
            for g in range(lots)
            for j in range(group)
        ],
        axis=0,
    )
    along_x = (dot(own.astype(BF), too[...]) + rim).reshape(ny, count, nx)
    slabs = [
        along_x[:, k * 8 : (k + 1) * 8, :].reshape(ny * 8, nx) for k in range(count // 8)
    ]
    result = dot(ky[...], jnp.concatenate(slabs, axis=1).astype(BF))
    starts = [first + i for first, size in blocks for i in range(0, size, 8)]
    for k, start in enumerate(starts):
        yield pl.ds(start, 8), result[:, k * nx : (k + 1) * nx].reshape(ny, 8, nx)


def kernel(
    ngx, ngz,
    view_ref, taps_ref, extents_ref, est_hbm, mea_hbm,
    out_ref,
    est_ref, mea_ref, table_ref,
    ext, side, packed, gathered, leaving, held, quot,
    mz, too, wide, ky,
    send_sem, recv_sem, all_send, all_recv, load_sem,
):
    load_est = pltpu.make_async_copy(est_hbm, est_ref, load_sem.at[0])
    load_mea = pltpu.make_async_copy(mea_hbm, mea_ref, load_sem.at[1])
    load_est.start()
    load_mea.start()
    ny, nz, nx = est_ref.shape
    planes = ny // ngz
    gx, gz = lax.axis_index("gx"), lax.axis_index("gz")
    has_x = {-1: gx > 0, 0: True, 1: gx < ngx - 1}
    has_z = {-1: gz > 0, 0: True, 1: gz < ngz - 1}

    def there(dx, dz):
        if dx == 0:
            return has_z[dz]
        if dz == 0:
            return has_x[dx]
        return jnp.logical_and(has_x[dx], has_z[dz])

    barrier = pltpu.get_barrier_semaphore()
    total = ngz - 1
    for d in range(1, ngz):
        pl.semaphore_signal(
            barrier, inc=1, device_id=(gx, lax.rem(gz + d, ngz)), device_id_type=MESH
        )
    for dx, dz in AROUND:
        if dx == 0:
            continue
        here = there(dx, dz)
        total = total + jnp.where(here, 1, 0)

        @pl.when(here)
        def _(dx=dx, dz=dz):
            pl.semaphore_signal(
                barrier, inc=1, device_id=(gx + dx, gz + dz), device_id_type=MESH
            )

    def landing(r, dx, dz):
        first, count = {-1: (0, PAD), 0: (PAD, nz), 1: (PAD + nz, PAD)}[dz]
        rows = pl.ds(first, count)
        if dx == 0:
            return ext.at[r, :, rows, :]
        return side.at[r, 0 if dx < 0 else 1, :, rows, :]

    def copy(r, dx, dz):
        first, count = {-1: (0, PAD), 0: (0, nz), 1: (nz - PAD, PAD)}[dz]
        if dx == 0:
            src = ext.at[r, :, pl.ds(PAD + first, count), :]
        else:
            src = packed.at[r, 0 if dx < 0 else 1, :, pl.ds(first, count), :]
        return pltpu.make_async_remote_copy(
            src_ref=src,
            dst_ref=landing(r, -dx, -dz),
            send_sem=send_sem.at[r, AROUND.index((dx, dz))],
            recv_sem=recv_sem.at[r, AROUND.index((-dx, -dz))],
            device_id=(gx + dx, gz + dz),
            device_id_type=MESH,
        )

    def arrival(r, dx, dz):
        first, count = {-1: (0, PAD), 0: (0, nz), 1: (nz - PAD, PAD)}[dz]
        dst = landing(r, dx, dz)
        return pltpu.make_async_remote_copy(
            src_ref=dst,
            dst_ref=dst,
            send_sem=send_sem.at[r, AROUND.index((dx, dz))],
            recv_sem=recv_sem.at[r, AROUND.index((dx, dz))],
            device_id=(gx + dx, gz + dz),
            device_id_type=MESH,
        )

    def clear(r):
        for dx, dz in AROUND:
            @pl.when(jnp.logical_not(there(dx, dz)))
            def _(dx=dx, dz=dz):
                spot = landing(r, dx, dz)
                spot[...] = jnp.zeros(spot.shape, BF)

    def send(r, which):
        for dx, dz in which:
            @pl.when(there(dx, dz))
            def _(dx=dx, dz=dz):
                copy(r, dx, dz).start()

    def receive(r, which):
        for dx, dz in which:
            @pl.when(there(dx, dz))
            def _(dx=dx, dz=dz):
                arrival(r, dx, dz).wait_recv()

    def sent(r):
        for dx, dz in AROUND:
            @pl.when(there(dx, dz))
            def _(dx=dx, dz=dz):
                copy(r, dx, dz).wait_send()

    above = [(0, -1), (0, 1)]
    sideways = [(-1, 0), (1, 0)]
    corners = [d for d in AROUND if d[0] and d[1]]
    middle = [(PAD, nz - 2 * PAD)]
    ends = [(0, PAD), (nz - PAD, PAD)]
    parts = middle + ends

    def exchange(d, part):
        to = lax.rem(gz + d, ngz)
        first, count = parts[part]
        there_rows = pl.ds(pl.multiple_of(gz * nz + first, PAD), count)
        return pltpu.make_async_remote_copy(
            src_ref=leaving.at[pl.ds(to * planes, planes), pl.ds(first, count), :],
            dst_ref=gathered.at[:, there_rows, :],
            send_sem=all_send.at[d, part],
            recv_sem=all_recv.at[d, part],
            device_id=(gx, to),
            device_id_type=MESH,
        )

    def blurred(r, blocks):
        if len(blocks) == 1:
            first, count = blocks[0]
            near = pl.ds(first, count + 2 * PAD)
            m = mz[r, 0:count, 0 : count + 2 * PAD]
        else:
            near = pl.ds(0, nz + 2 * PAD)
            m = jnp.concatenate([mz[r, first : first + count, :] for first, count in blocks], axis=0)
        yield from blur_rows(
            blocks, near, m, ext.at[r], side.at[r], too.at[r], wide.at[r], ky.at[r], ny, nx
        )

    def quotients(blocks):
        for rows, value in blurred(0, blocks):
            quot[:, rows, :] = mea_ref[:, rows, :] / value
        for first, count in blocks:
            ext[1, :, PAD + first : PAD + first + count, :] = quot[
                :, first : first + count, :
            ].astype(BF)

    def products(blocks):
        for rows, value in blurred(1, blocks):
            held[:, rows, :] = est_ref[:, rows, :] * value
        for first, count in blocks:
            rows = slice(first, first + count)
            leaving[:, rows, :] = held[:, rows, :].astype(BF)

    load_est.wait()
    ext[0, :, PAD : PAD + nz, :] = est_ref[...].astype(BF)
    pl.semaphore_wait(barrier, total)
    send(0, above)
    pack_edges(lambda y: est_ref[y], packed.at[0], ny, nz, nx)
    send(0, corners + sideways)
    view = view_ref[0]
    for flip in range(2):
        make_matrices(
            taps_ref, view, extents_ref, bool(flip),
            mz.at[flip], too.at[flip], wide.at[flip], ky.at[flip], ny, nz, nx,
        )
    clear(0)
    clear(1)
    load_mea.wait()
    receive(0, sideways)
    quotients(middle)
    receive(0, above + corners)
    quotients(ends)
    send(1, above)
    pack_edges(lambda y: quot[y], packed.at[1], ny, nz, nx)
    send(1, corners + sideways)
    make_table(table_ref, nz * ngz)
    receive(1, sideways)
    products(middle)
    for d in range(1, ngz):
        exchange(d, 0).start()
    receive(1, above + corners)
    products(ends)
    for d in range(1, ngz):
        for part in (1, 2):
            exchange(d, part).start()
    mine = pl.ds(pl.multiple_of(gz * nz, nz), nz)
    gathered[:, mine, :] = leaving[pl.ds(gz * planes, planes)]
    for d in range(1, ngz):
        for part in range(3):
            exchange(d, part).wait_recv()
    lines = jnp.concatenate([gathered[y] for y in range(planes)], axis=1)
    step = nz * ngz
    for b in range(UP):
        rows = slice(b * step, (b + 1) * step)
        whole = dot(table_ref[rows, :], lines)
        for y in range(planes):
            out_ref[y, rows, :] = whole[:, y * nx : (y + 1) * nx]
    sent(0)
    sent(1)
    for d in range(1, ngz):
        for part in range(3):
            exchange(d, part).wait_send()


def on_device(ngx, ngz, view_index, psf_taps, extents, estimate, measured):
    ny, nz, nx = estimate.shape
    planes, lines = ny // ngz, nz * ngz
    group = nx // PAD
    smem = pl.BlockSpec(memory_space=pltpu.SMEM)
    vmem = pl.BlockSpec(memory_space=pltpu.VMEM)
    anywhere = pl.BlockSpec(memory_space=pl.ANY)
    return pl.pallas_call(
        functools.partial(kernel, ngx, ngz),
        out_shape=pltpu.VMEM((planes, UP * lines, nx), F32),
        in_specs=[smem, smem, smem, anywhere, anywhere],
        out_specs=vmem,
        scratch_shapes=[
            pltpu.VMEM((ny, nz, nx), F32),
            pltpu.VMEM((ny, nz, nx), F32),
            pltpu.VMEM((UP * lines, lines), BF),
            pltpu.VMEM((2, ny, nz + 2 * PAD, nx), BF),
            pltpu.VMEM((2, 2, ny // group, nz + 2 * PAD, nx), BF),
            pltpu.VMEM((2, 2, ny // group, nz, nx), BF),
            pltpu.VMEM((planes, lines, nx), BF),
            pltpu.VMEM((ny, nz, nx), BF),
            pltpu.VMEM((ny, nz, nx), F32),
            pltpu.VMEM((ny, nz, nx), F32),
            pltpu.VMEM((2, nz, nz + 2 * PAD), BF),
            pltpu.VMEM((2, nx, nx), BF),
            pltpu.VMEM((2, 2 * nx, group * nx), BF),
            pltpu.VMEM((2, ny * 8, ny * 8), BF),
            pltpu.SemaphoreType.DMA((2, 8)),
            pltpu.SemaphoreType.DMA((2, 8)),
            pltpu.SemaphoreType.DMA((ngz, 3)),
            pltpu.SemaphoreType.DMA((ngz, 3)),
            pltpu.SemaphoreType.DMA((2,)),
        ],
        compiler_params=pltpu.CompilerParams(collective_id=0, has_side_effects=True),
    )(view_index, psf_taps, extents.T, estimate, measured)


def solution(mesh):
    return jax.shard_map(
        functools.partial(on_device, mesh.shape["gx"], mesh.shape["gz"]),
        mesh=mesh,
        in_specs=(P(), P(), P(), P(None, "gz", "gx"), P(None, "gz", "gx")),
        out_specs=P("gz", None, "gx"),
        check_vma=False,
    )
```

```python
import functools

import jax
import jax.numpy as jnp
from jax import lax
from jax.experimental import pallas as pl
from jax.experimental.pallas import tpu as pltpu
from jax.sharding import PartitionSpec as P

HALF = 15
TAPS = 31
UP = 4
PAD = 16
BF = jnp.bfloat16
F32 = jnp.float32
MESH = pl.DeviceIdType.MESH
AROUND = [(dx, dz) for dz in (-1, 1, 0) for dx in (0, -1, 1) if (dx, dz) != (0, 0)]


def dot(a, b):
    return jnp.dot(a, b, preferred_element_type=F32)


def lanes_of(shape):
    return lax.broadcasted_iota(jnp.int32, shape, 1)


def rows_of(shape):
    return lax.broadcasted_iota(jnp.int32, shape, 0)


def tap_row(taps_ref, view, extents_ref, axis_id, width, spread, flip):
    lane = lanes_of((8, width))
    row = jnp.zeros((8, width), F32)
    for t in range(TAPS):
        spot = (TAPS - 1 - t if flip else t) * spread
        row = jnp.where(lane == spot, taps_ref[view, axis_id, t], row)
    keep = jnp.abs(lane - HALF * spread) <= extents_ref[axis_id, view] * spread
    row = jnp.where(keep, row, 0.0)
    return row / jnp.sum(row, axis=1, keepdims=True)


def slanted(row, count, shift):
    width = row.shape[1]
    tall = jnp.broadcast_to(row[0:1], (count, width))
    return pltpu.roll(tall, shift % width, 1, stride=1, stride_axis=0)


def make_matrices(taps_ref, view, extents_ref, flip, mz, too, wide, ky, ny, nz, nx):
    group = nx // PAD
    if flip:
        lines = mz.shape[0]
        full = slanted(tap_row(taps_ref, view, extents_ref, 2, lines, 1, flip), lines, -HALF)
        away = jnp.abs(lanes_of((lines, lines)) - rows_of((lines, lines)))
        mz[...] = jnp.where(away <= HALF, full, 0.0).astype(BF)
    else:
        mz[...] = slanted(tap_row(taps_ref, view, extents_ref, 2, nx, 1, flip), nz, 1)[
            :, : nz + 2 * PAD
        ].astype(BF)
    ring = slanted(tap_row(taps_ref, view, extents_ref, 0, nx, 1, not flip), nx, -HALF)
    lane, row = lanes_of((nx, nx)), rows_of((nx, nx))
    too[...] = jnp.where(jnp.abs(lane - row) <= HALF, ring, 0.0).astype(BF)
    edge = lanes_of((PAD, nx))
    from_left = jnp.where(edge < nx // 2, ring[nx - PAD :], 0.0).astype(BF)
    from_right = jnp.where(edge >= nx // 2, ring[:PAD], 0.0).astype(BF)
    wide[...] = jnp.zeros(wide.shape, BF)
    for j in range(group):
        wide[j * PAD : (j + 1) * PAD, j * nx : (j + 1) * nx] = from_left
        wide[nx + j * PAD : nx + (j + 1) * PAD, j * nx : (j + 1) * nx] = from_right
    sub = 8
    long = tap_row(taps_ref, view, extents_ref, 1, 2 * ny * sub, sub, flip)
    ky[...] = slanted(long, ny * sub, -HALF * sub)[:, : ny * sub].astype(BF)


def make_table(table, length):
    shape = (PAD, length)
    offset = jnp.bitwise_and(rows_of(shape) - UP * lanes_of(shape), UP * length - 1)
    sine = jnp.sin(jnp.pi * jnp.bitwise_and(offset, 2 * UP - 1).astype(F32) / UP)
    angle = jnp.pi * offset.astype(F32) / (UP * length)
    on_grid = jnp.bitwise_and(offset, UP - 1) == 0
    below = jnp.where(on_grid, 1.0, length * jnp.sin(angle) / jnp.where(on_grid, 1.0, jnp.cos(angle)))
    first = jnp.where(on_grid, jnp.where(offset == 0, 1.0, 0.0), sine / below)

    for j in range(UP * length // PAD):
        moved = pltpu.roll(first, j * (PAD // UP), 1) if j else first
        table[j * PAD : (j + 1) * PAD, :] = moved.astype(BF)


def pack_edges(volume, packed, ny, nz, nx):
    group = nx // PAD
    lane = lanes_of((nz, nx)) // PAD
    for g in range(ny // group):
        left = right = None
        for j in range(group):
            plane = volume(g * group + j)
            a = pltpu.roll(plane, (j * PAD) % nx, 1) if j else plane
            s = (j * PAD - (nx - PAD)) % nx
            b = pltpu.roll(plane, s, 1) if s else plane
            left = a if left is None else jnp.where(lane == j, a, left)
            right = b if right is None else jnp.where(lane == j, b, right)
        packed[0, g] = left.astype(BF)
        packed[1, g] = right.astype(BF)


def passes_xy(own, rim, too, wide, ky, ny, count, nx):
    group = nx // PAD
    lots = ny // group
    rim = dot(rim, wide[...])
    rim = jnp.concatenate(
        [
            rim[g * count : (g + 1) * count, j * nx : (j + 1) * nx]
            for g in range(lots)
            for j in range(group)
        ],
        axis=0,
    )
    along_x = (dot(own, too[...]) + rim).reshape(ny, count, nx)
    slabs = [
        along_x[:, k * 8 : (k + 1) * 8, :].reshape(ny * 8, nx) for k in range(count // 8)
    ]
    return dot(ky[...], jnp.concatenate(slabs, axis=1).astype(BF))


def blur_rows(blocks, near, m, ext, side, too, wide, ky, ny, nx):
    group = nx // PAD
    lots = ny // group
    count = m.shape[0]
    lines = [ext[y, near, :] for y in range(ny)]
    lines += [side[q, g, near, :] for g in range(lots) for q in range(2)]
    along_z = dot(m, jnp.concatenate(lines, axis=1))
    own = jnp.concatenate([along_z[:, y * nx : (y + 1) * nx] for y in range(ny)], axis=0)
    rim = jnp.concatenate(
        [along_z[:, (ny + 2 * g) * nx : (ny + 2 * g + 2) * nx] for g in range(lots)], axis=0
    )
    result = passes_xy(own.astype(BF), rim.astype(BF), too, wide, ky, ny, count, nx)
    starts = [first + i for first, size in blocks for i in range(0, size, 8)]
    for k, start in enumerate(starts):
        yield pl.ds(start, 8), result[:, k * nx : (k + 1) * nx].reshape(ny, 8, nx)


def kernel(
    ngx, ngz,
    view_ref, taps_ref, extents_ref, est_hbm, mea_hbm,
    out_ref,
    est_ref, mea_ref, table_ref,
    ext, side, packed, quot, rim_out, rim_in, leaving, gathered, est_lines,
    mz, mz_all, too, wide, ky,
    send_sem, recv_sem, rim_send, rim_recv, all_send, all_recv, load_sem,
):
    load_est = pltpu.make_async_copy(est_hbm, est_ref, load_sem.at[0])
    load_mea = pltpu.make_async_copy(mea_hbm, mea_ref, load_sem.at[1])
    load_est.start()
    load_mea.start()
    ny, nz, nx = est_ref.shape
    planes = ny // ngz
    gx, gz = lax.axis_index("gx"), lax.axis_index("gz")
    has_x = {-1: gx > 0, 0: True, 1: gx < ngx - 1}
    has_z = {-1: gz > 0, 0: True, 1: gz < ngz - 1}

    def there(dx, dz):
        if dx == 0:
            return has_z[dz]
        if dz == 0:
            return has_x[dx]
        return jnp.logical_and(has_x[dx], has_z[dz])

    barrier = pltpu.get_barrier_semaphore()
    total = ngz - 1
    for d in range(1, ngz):
        pl.semaphore_signal(
            barrier, inc=1, device_id=(gx, lax.rem(gz + d, ngz)), device_id_type=MESH
        )
    for dx, dz in AROUND:
        if dx == 0:
            continue
        here = there(dx, dz)
        total = total + jnp.where(here, 1, 0)

        @pl.when(here)
        def _(dx=dx, dz=dz):
            pl.semaphore_signal(
                barrier, inc=1, device_id=(gx + dx, gz + dz), device_id_type=MESH
            )

    def landing(r, dx, dz):
        first, count = {-1: (0, PAD), 0: (PAD, nz), 1: (PAD + nz, PAD)}[dz]
        rows = pl.ds(first, count)
        if dx == 0:
            return ext.at[:, rows, :]
        return side.at[0 if dx < 0 else 1, :, rows, :]

    def copy(r, dx, dz):
        first, count = {-1: (0, PAD), 0: (0, nz), 1: (nz - PAD, PAD)}[dz]
        if dx == 0:
            src = ext.at[:, pl.ds(PAD + first, count), :]
        else:
            src = packed.at[0 if dx < 0 else 1, :, pl.ds(first, count), :]
        return pltpu.make_async_remote_copy(
            src_ref=src,
            dst_ref=landing(r, -dx, -dz),
            send_sem=send_sem.at[AROUND.index((dx, dz))],
            recv_sem=recv_sem.at[AROUND.index((-dx, -dz))],
            device_id=(gx + dx, gz + dz),
            device_id_type=MESH,
        )

    def arrival(r, dx, dz):
        first, count = {-1: (0, PAD), 0: (0, nz), 1: (nz - PAD, PAD)}[dz]
        dst = landing(r, dx, dz)
        return pltpu.make_async_remote_copy(
            src_ref=dst,
            dst_ref=dst,
            send_sem=send_sem.at[AROUND.index((dx, dz))],
            recv_sem=recv_sem.at[AROUND.index((dx, dz))],
            device_id=(gx + dx, gz + dz),
            device_id_type=MESH,
        )

    def clear(r):
        for dx, dz in AROUND:
            @pl.when(jnp.logical_not(there(dx, dz)))
            def _(dx=dx, dz=dz):
                spot = landing(r, dx, dz)
                spot[...] = jnp.zeros(spot.shape, BF)

    def send(r, which):
        for dx, dz in which:
            @pl.when(there(dx, dz))
            def _(dx=dx, dz=dz):
                copy(r, dx, dz).start()

    def receive(r, which):
        for dx, dz in which:
            @pl.when(there(dx, dz))
            def _(dx=dx, dz=dz):
                arrival(r, dx, dz).wait_recv()

    def sent(r):
        for dx, dz in AROUND:
            @pl.when(there(dx, dz))
            def _(dx=dx, dz=dz):
                copy(r, dx, dz).wait_send()

    above = [(0, -1), (0, 1)]
    sideways = [(-1, 0), (1, 0)]
    corners = [d for d in AROUND if d[0] and d[1]]
    parts = [[(PAD, nz - 2 * PAD)], [(0, PAD), (nz - PAD, PAD)]]
    counts = [nz - 2 * PAD, 2 * PAD]
    lots = packed.shape[1]

    def rim_copy(p, dx):
        rows = pl.ds(0, counts[p])
        return pltpu.make_async_remote_copy(
            src_ref=rim_out.at[p, 0 if dx < 0 else 1, :, rows, :],
            dst_ref=rim_in.at[p, 1 if dx < 0 else 0, :, rows, :],
            send_sem=rim_send.at[p, 0 if dx < 0 else 1],
            recv_sem=rim_recv.at[p, 1 if dx < 0 else 0],
            device_id=(gx + dx, gz),
            device_id_type=MESH,
        )

    def rim_arrival(p, dx):
        dst = rim_in.at[p, 0 if dx < 0 else 1, :, pl.ds(0, counts[p]), :]
        return pltpu.make_async_remote_copy(
            src_ref=dst,
            dst_ref=dst,
            send_sem=rim_send.at[p, 0 if dx < 0 else 1],
            recv_sem=rim_recv.at[p, 0 if dx < 0 else 1],
            device_id=(gx + dx, gz),
            device_id_type=MESH,
        )

    def exchange(d, p):
        to = lax.rem(gz + d, ngz)
        theirs = pl.ds(to * planes, planes)
        if p == 2:
            src = est_out(theirs)
            dst = est_lines.at[:, pl.ds(pl.multiple_of(gz * nz, nz), nz), :]
        else:
            src = leaving.at[p, theirs, pl.ds(0, counts[p]), :]
            dst = gathered.at[p, gz, :, pl.ds(0, counts[p]), :]
        return pltpu.make_async_remote_copy(
            src_ref=src,
            dst_ref=dst,
            send_sem=all_send.at[d, p],
            recv_sem=all_recv.at[d, p],
            device_id=(gx, to),
            device_id_type=MESH,
        )

    def est_out(which):
        return ext.at[which, pl.ds(PAD, nz), :]

    def quotients(p):
        blocks = parts[p]
        if p == 0:
            first, count = blocks[0]
            near = pl.ds(first, count + 2 * PAD)
            m = mz[0:count, 0 : count + 2 * PAD]
        else:
            near = pl.ds(0, nz + 2 * PAD)
            m = jnp.concatenate([mz[first : first + count, :] for first, count in blocks], axis=0)
        at = 0
        for rows, value in blur_rows(
            blocks, near, m, ext, side, too.at[0], wide.at[0], ky.at[0], ny, nx
        ):
            quot[p, :, at : at + 8, :] = mea_ref[:, rows, :] / value
            at += 8
        count = counts[p]
        pack_edges(
            lambda y: quot[p, y, :count, :], rim_out.at[p, :, :, pl.ds(0, count), :], ny, count, nx
        )
        for dx in (-1, 1):
            @pl.when(has_x[dx])
            def _(dx=dx):
                rim_copy(p, dx).start()

            @pl.when(jnp.logical_not(has_x[dx]))
            def _(dx=dx):
                spot = rim_in.at[p, 0 if dx < 0 else 1]
                spot[...] = jnp.zeros(spot.shape, BF)

    def regroup(p):
        for dx in (-1, 1):
            @pl.when(has_x[dx])
            def _(dx=dx):
                rim_arrival(p, dx).wait_recv()
        count = counts[p]
        own = quot[p, :, :count, :].reshape(ny * count, nx).astype(BF)
        rim = jnp.concatenate(
            [
                jnp.concatenate([rim_in[p, q, g, :count, :] for q in range(2)], axis=1)
                for g in range(lots)
            ],
            axis=0,
        )
        result = passes_xy(own, rim, too.at[1], wide.at[1], ky.at[1], ny, count, nx)
        for k in range(count // PAD):
            pair = [
                result[:, i * nx : (i + 1) * nx].reshape(ny, 8, nx) for i in (2 * k, 2 * k + 1)
            ]
            leaving[p, :, k * PAD : (k + 1) * PAD, :] = jnp.concatenate(pair, axis=1).astype(BF)
        for d in range(1, ngz):
            exchange(d, p).start()
        gathered[p, gz, :, :count, :] = leaving[p, pl.ds(gz * planes, planes), :count, :]

    load_est.wait()
    ext[:, PAD : PAD + nz, :] = est_ref[...].astype(BF)
    pl.semaphore_wait(barrier, total)
    send(0, above)
    pack_edges(lambda y: est_ref[y], packed, ny, nz, nx)
    send(0, corners + sideways)
    for d in range(1, ngz):
        exchange(d, 2).start()
    view = view_ref[0]
    for flip in range(2):
        make_matrices(
            taps_ref, view, extents_ref, bool(flip),
            mz_all if flip else mz, too.at[flip], wide.at[flip], ky.at[flip], ny, nz, nx,
        )
    clear(0)
    load_mea.wait()
    receive(0, sideways)
    quotients(0)
    make_table(table_ref, nz * ngz)
    est_lines[:, pl.ds(pl.multiple_of(gz * nz, nz), nz), :] = ext[
        pl.ds(gz * planes, planes), PAD : PAD + nz, :
    ]
    regroup(0)
    receive(0, above + corners)
    quotients(1)
    regroup(1)
    for d in range(1, ngz):
        for p in (2, 0, 1):
            exchange(d, p).wait_recv()
    lines = []
    for y in range(planes):
        line = []
        for g in range(ngz):
            line += [
                gathered[1, g, y, :PAD, :],
                gathered[0, g, y, : counts[0], :],
                gathered[1, g, y, PAD : 2 * PAD, :],
            ]
        lines.append(jnp.concatenate(line, axis=0))
    correction = dot(mz_all[...], jnp.concatenate(lines, axis=1))
    estimate = jnp.concatenate([est_lines[y] for y in range(planes)], axis=1)
    rounded = (estimate.astype(F32) * correction).astype(BF)
    step = nz * ngz
    for b in range(UP):
        rows = slice(b * step, (b + 1) * step)
        whole = dot(table_ref[rows, :], rounded)
        for y in range(planes):
            out_ref[y, rows, :] = whole[:, y * nx : (y + 1) * nx]
    sent(0)
    for p in range(2):
        for dx in (-1, 1):
            @pl.when(has_x[dx])
            def _(p=p, dx=dx):
                rim_copy(p, dx).wait_send()
    for d in range(1, ngz):
        for p in range(3):
            exchange(d, p).wait_send()


def on_device(ngx, ngz, view_index, psf_taps, extents, estimate, measured):
    ny, nz, nx = estimate.shape
    planes, lines = ny // ngz, nz * ngz
    group = nx // PAD
    half = max(2 * PAD, nz - 2 * PAD)
    smem = pl.BlockSpec(memory_space=pltpu.SMEM)
    vmem = pl.BlockSpec(memory_space=pltpu.VMEM)
    anywhere = pl.BlockSpec(memory_space=pl.ANY)
    return pl.pallas_call(
        functools.partial(kernel, ngx, ngz),
        out_shape=pltpu.VMEM((planes, UP * lines, nx), F32),
        in_specs=[smem, smem, smem, anywhere, anywhere],
        out_specs=vmem,
        scratch_shapes=[
            pltpu.VMEM((ny, nz, nx), F32),
            pltpu.VMEM((ny, nz, nx), F32),
            pltpu.VMEM((UP * lines, lines), BF),
            pltpu.VMEM((ny, nz + 2 * PAD, nx), BF),
            pltpu.VMEM((2, ny // group, nz + 2 * PAD, nx), BF),
            pltpu.VMEM((2, ny // group, nz, nx), BF),
            pltpu.VMEM((2, ny, half, nx), F32),
            pltpu.VMEM((2, 2, ny // group, half, nx), BF),
            pltpu.VMEM((2, 2, ny // group, half, nx), BF),
            pltpu.VMEM((2, ny, half, nx), BF),
            pltpu.VMEM((2, ngz, planes, half, nx), BF),
            pltpu.VMEM((planes, lines, nx), BF),
            pltpu.VMEM((nz, nz + 2 * PAD), BF),
            pltpu.VMEM((lines, lines), BF),
            pltpu.VMEM((2, nx, nx), BF),
            pltpu.VMEM((2, 2 * nx, group * nx), BF),
            pltpu.VMEM((2, ny * 8, ny * 8), BF),
            pltpu.SemaphoreType.DMA((8,)),
            pltpu.SemaphoreType.DMA((8,)),
            pltpu.SemaphoreType.DMA((2, 2)),
            pltpu.SemaphoreType.DMA((2, 2)),
            pltpu.SemaphoreType.DMA((ngz, 3)),
            pltpu.SemaphoreType.DMA((ngz, 3)),
            pltpu.SemaphoreType.DMA((2,)),
        ],
        compiler_params=pltpu.CompilerParams(collective_id=0, has_side_effects=True),
    )(view_index, psf_taps, extents.T, estimate, measured)


def solution(mesh):
    return jax.shard_map(
        functools.partial(on_device, mesh.shape["gx"], mesh.shape["gz"]),
        mesh=mesh,
        in_specs=(P(), P(), P(), P(None, "gz", "gx"), P(None, "gz", "gx")),
        out_specs=P("gz", None, "gx"),
        check_vma=False,
    )
```

```python
import functools

import jax
import jax.numpy as jnp
from jax import lax
from jax.experimental import pallas as pl
from jax.experimental.pallas import tpu as pltpu
from jax.sharding import PartitionSpec as P

HALF = 15
TAPS = 31
UP = 4
PAD = 16
BF = jnp.bfloat16
F32 = jnp.float32
MESH = pl.DeviceIdType.MESH
AROUND = [(dx, dz) for dz in (-1, 1, 0) for dx in (0, -1, 1) if (dx, dz) != (0, 0)]


def dot(a, b):
    return jnp.dot(a, b, preferred_element_type=F32)


def lanes_of(shape):
    return lax.broadcasted_iota(jnp.int32, shape, 1)


def rows_of(shape):
    return lax.broadcasted_iota(jnp.int32, shape, 0)


def tap_row(taps_ref, view, extents_ref, axis_id, width, spread, flip):
    lane = lanes_of((8, width))
    row = jnp.zeros((8, width), F32)
    for t in range(TAPS):
        spot = (TAPS - 1 - t if flip else t) * spread
        row = jnp.where(lane == spot, taps_ref[view, axis_id, t], row)
    keep = jnp.abs(lane - HALF * spread) <= extents_ref[axis_id, view] * spread
    row = jnp.where(keep, row, 0.0)
    return row / jnp.sum(row, axis=1, keepdims=True)


def slanted(row, count, shift):
    width = row.shape[1]
    tall = jnp.broadcast_to(row[0:1], (count, width))
    return pltpu.roll(tall, shift % width, 1, stride=1, stride_axis=0)


def make_matrices(taps_ref, view, extents_ref, flip, mz, too, wide, ky, ny, nz, nx):
    group = nx // PAD
    if flip:
        lines = mz.shape[0]
        full = slanted(tap_row(taps_ref, view, extents_ref, 2, lines, 1, flip), lines, -HALF)
        away = jnp.abs(lanes_of((lines, lines)) - rows_of((lines, lines)))
        mz[...] = jnp.where(away <= HALF, full, 0.0).astype(BF)
    else:
        mz[...] = slanted(tap_row(taps_ref, view, extents_ref, 2, nx, 1, flip), nz, 1)[
            :, : nz + 2 * PAD
        ].astype(BF)
    ring = slanted(tap_row(taps_ref, view, extents_ref, 0, nx, 1, not flip), nx, -HALF)
    lane, row = lanes_of((nx, nx)), rows_of((nx, nx))
    too[...] = jnp.where(jnp.abs(lane - row) <= HALF, ring, 0.0).astype(BF)
    edge = lanes_of((PAD, nx))
    from_left = jnp.where(edge < nx // 2, ring[nx - PAD :], 0.0).astype(BF)
    from_right = jnp.where(edge >= nx // 2, ring[:PAD], 0.0).astype(BF)
    wide[...] = jnp.zeros(wide.shape, BF)
    for j in range(group):
        wide[j * PAD : (j + 1) * PAD, j * nx : (j + 1) * nx] = from_left
        wide[nx + j * PAD : nx + (j + 1) * PAD, j * nx : (j + 1) * nx] = from_right
    sub = 8
    long = tap_row(taps_ref, view, extents_ref, 1, 2 * ny * sub, sub, flip)
    ky[...] = slanted(long, ny * sub, -HALF * sub)[:, : ny * sub].astype(BF)


def make_table(table, length):
    shape = (PAD, length)
    offset = jnp.bitwise_and(rows_of(shape) - UP * lanes_of(shape), UP * length - 1)
    sine = jnp.sin(jnp.pi * jnp.bitwise_and(offset, 2 * UP - 1).astype(F32) / UP)
    angle = jnp.pi * offset.astype(F32) / (UP * length)
    on_grid = jnp.bitwise_and(offset, UP - 1) == 0
    below = jnp.where(on_grid, 1.0, length * jnp.sin(angle) / jnp.where(on_grid, 1.0, jnp.cos(angle)))
    first = jnp.where(on_grid, jnp.where(offset == 0, 1.0, 0.0), sine / below)

    for j in range(UP * length // PAD):
        moved = pltpu.roll(first, j * (PAD // UP), 1) if j else first
        table[j * PAD : (j + 1) * PAD, :] = moved.astype(BF)


def pack_edges(volume, packed, ny, nz, nx):
    group = nx // PAD
    lane = lanes_of((nz, nx)) // PAD
    for g in range(ny // group):
        left = right = None
        for j in range(group):
            plane = volume(g * group + j)
            a = pltpu.roll(plane, (j * PAD) % nx, 1) if j else plane
            s = (j * PAD - (nx - PAD)) % nx
            b = pltpu.roll(plane, s, 1) if s else plane
            left = a if left is None else jnp.where(lane == j, a, left)
            right = b if right is None else jnp.where(lane == j, b, right)
        packed[0, g] = left.astype(BF)
        packed[1, g] = right.astype(BF)


def passes_xy(own, rim, too, wide, ky, ny, count, nx):
    group = nx // PAD
    lots = ny // group
    rim = dot(rim, wide[...])
    rim = jnp.concatenate(
        [
            rim[g * count : (g + 1) * count, j * nx : (j + 1) * nx]
            for g in range(lots)
            for j in range(group)
        ],
        axis=0,
    )
    along_x = (dot(own, too[...]) + rim).reshape(ny, count, nx)
    slabs = [
        along_x[:, k * 8 : (k + 1) * 8, :].reshape(ny * 8, nx) for k in range(count // 8)
    ]
    return dot(ky[...], jnp.concatenate(slabs, axis=1).astype(BF))


def blur_rows(blocks, near, m, ext, side, too, wide, ky, ny, nx):
    group = nx // PAD
    lots = ny // group
    count = m.shape[0]
    lines = [ext[y, near, :] for y in range(ny)]
    lines += [side[q, g, near, :] for g in range(lots) for q in range(2)]
    along_z = dot(m, jnp.concatenate(lines, axis=1))
    own = jnp.concatenate([along_z[:, y * nx : (y + 1) * nx] for y in range(ny)], axis=0)
    rim = jnp.concatenate(
        [along_z[:, (ny + 2 * g) * nx : (ny + 2 * g + 2) * nx] for g in range(lots)], axis=0
    )
    result = passes_xy(own.astype(BF), rim.astype(BF), too, wide, ky, ny, count, nx)
    starts = [first + i for first, size in blocks for i in range(0, size, 8)]
    for k, start in enumerate(starts):
        yield pl.ds(start, 8), result[:, k * nx : (k + 1) * nx].reshape(ny, 8, nx)


def kernel(
    ngx, ngz,
    view_ref, taps_ref, extents_ref, est_hbm, mea_hbm,
    out_ref,
    est_ref, mea_ref, table_ref,
    ext, side, packed, quot, rim_out, rim_in, leaving, gathered, est_lines,
    mz, mz_all, too, wide, ky,
    send_sem, recv_sem, rim_send, rim_recv, all_send, all_recv, load_sem,
):
    load_est = pltpu.make_async_copy(est_hbm, est_ref, load_sem.at[0])
    load_mea = pltpu.make_async_copy(mea_hbm, mea_ref, load_sem.at[1])
    load_est.start()
    load_mea.start()
    ny, nz, nx = est_ref.shape
    planes = ny // ngz
    gx, gz = lax.axis_index("gx"), lax.axis_index("gz")
    has_x = {-1: gx > 0, 0: True, 1: gx < ngx - 1}
    has_z = {-1: gz > 0, 0: True, 1: gz < ngz - 1}

    def there(dx, dz):
        if dx == 0:
            return has_z[dz]
        if dz == 0:
            return has_x[dx]
        return jnp.logical_and(has_x[dx], has_z[dz])

    barrier = pltpu.get_barrier_semaphore()
    total = ngz - 1
    for d in range(1, ngz):
        pl.semaphore_signal(
            barrier, inc=1, device_id=(gx, lax.rem(gz + d, ngz)), device_id_type=MESH
        )
    for dx, dz in AROUND:
        if dx == 0:
            continue
        here = there(dx, dz)
        total = total + jnp.where(here, 1, 0)

        @pl.when(here)
        def _(dx=dx, dz=dz):
            pl.semaphore_signal(
                barrier, inc=1, device_id=(gx + dx, gz + dz), device_id_type=MESH
            )

    def landing(r, dx, dz):
        first, count = {-1: (0, PAD), 0: (PAD, nz), 1: (PAD + nz, PAD)}[dz]
        rows = pl.ds(first, count)
        if dx == 0:
            return ext.at[:, rows, :]
        return side.at[0 if dx < 0 else 1, :, rows, :]

    def copy(r, dx, dz):
        first, count = {-1: (0, PAD), 0: (0, nz), 1: (nz - PAD, PAD)}[dz]
        if dx == 0:
            src = ext.at[:, pl.ds(PAD + first, count), :]
        else:
            src = packed.at[0 if dx < 0 else 1, :, pl.ds(first, count), :]
        return pltpu.make_async_remote_copy(
            src_ref=src,
            dst_ref=landing(r, -dx, -dz),
            send_sem=send_sem.at[AROUND.index((dx, dz))],
            recv_sem=recv_sem.at[AROUND.index((-dx, -dz))],
            device_id=(gx + dx, gz + dz),
            device_id_type=MESH,
        )

    def arrival(r, dx, dz):
        first, count = {-1: (0, PAD), 0: (0, nz), 1: (nz - PAD, PAD)}[dz]
        dst = landing(r, dx, dz)
        return pltpu.make_async_remote_copy(
            src_ref=dst,
            dst_ref=dst,
            send_sem=send_sem.at[AROUND.index((dx, dz))],
            recv_sem=recv_sem.at[AROUND.index((dx, dz))],
            device_id=(gx + dx, gz + dz),
            device_id_type=MESH,
        )

    def clear(r):
        for dx, dz in AROUND:
            @pl.when(jnp.logical_not(there(dx, dz)))
            def _(dx=dx, dz=dz):
                spot = landing(r, dx, dz)
                spot[...] = jnp.zeros(spot.shape, BF)

    def send(r, which):
        for dx, dz in which:
            @pl.when(there(dx, dz))
            def _(dx=dx, dz=dz):
                copy(r, dx, dz).start()

    def receive(r, which):
        for dx, dz in which:
            @pl.when(there(dx, dz))
            def _(dx=dx, dz=dz):
                arrival(r, dx, dz).wait_recv()

    def sent(r):
        for dx, dz in AROUND:
            @pl.when(there(dx, dz))
            def _(dx=dx, dz=dz):
                copy(r, dx, dz).wait_send()

    above = [(0, -1), (0, 1)]
    sideways = [(-1, 0), (1, 0)]
    corners = [d for d in AROUND if d[0] and d[1]]
    parts = [[(PAD, nz - 2 * PAD)], [(0, PAD), (nz - PAD, PAD)]]
    counts = [nz - 2 * PAD, 2 * PAD]
    lots = packed.shape[1]

    def rim_copy(p, dx):
        rows = pl.ds(0, counts[p])
        return pltpu.make_async_remote_copy(
            src_ref=rim_out.at[p, 0 if dx < 0 else 1, :, rows, :],
            dst_ref=rim_in.at[p, 1 if dx < 0 else 0, :, rows, :],
            send_sem=rim_send.at[p, 0 if dx < 0 else 1],
            recv_sem=rim_recv.at[p, 1 if dx < 0 else 0],
            device_id=(gx + dx, gz),
            device_id_type=MESH,
        )

    def rim_arrival(p, dx):
        dst = rim_in.at[p, 0 if dx < 0 else 1, :, pl.ds(0, counts[p]), :]
        return pltpu.make_async_remote_copy(
            src_ref=dst,
            dst_ref=dst,
            send_sem=rim_send.at[p, 0 if dx < 0 else 1],
            recv_sem=rim_recv.at[p, 0 if dx < 0 else 1],
            device_id=(gx + dx, gz),
            device_id_type=MESH,
        )

    def exchange(d, p):
        to = lax.rem(gz + d, ngz)
        theirs = pl.ds(to * planes, planes)
        if p == 2:
            src = est_out(theirs)
            dst = est_lines.at[:, pl.ds(pl.multiple_of(gz * nz, nz), nz), :]
        else:
            src = leaving.at[p, theirs, pl.ds(0, counts[p]), :]
            dst = gathered.at[p, gz, :, pl.ds(0, counts[p]), :]
        return pltpu.make_async_remote_copy(
            src_ref=src,
            dst_ref=dst,
            send_sem=all_send.at[d, p],
            recv_sem=all_recv.at[d, p],
            device_id=(gx, to),
            device_id_type=MESH,
        )

    def est_out(which):
        return ext.at[which, pl.ds(PAD, nz), :]

    def quotients(p):
        blocks = parts[p]
        if p == 0:
            first, count = blocks[0]
            near = pl.ds(first, count + 2 * PAD)
            m = mz[0:count, 0 : count + 2 * PAD]
        else:
            near = pl.ds(0, nz + 2 * PAD)
            m = jnp.concatenate([mz[first : first + count, :] for first, count in blocks], axis=0)
        at = 0
        for rows, value in blur_rows(
            blocks, near, m, ext, side, too.at[0], wide.at[0], ky.at[0], ny, nx
        ):
            quot[p, :, at : at + 8, :] = mea_ref[:, rows, :] / value
            at += 8
        count = counts[p]
        pack_edges(
            lambda y: quot[p, y, :count, :], rim_out.at[p, :, :, pl.ds(0, count), :], ny, count, nx
        )
        for dx in (-1, 1):
            @pl.when(has_x[dx])
            def _(dx=dx):
                rim_copy(p, dx).start()

            @pl.when(jnp.logical_not(has_x[dx]))
            def _(dx=dx):
                spot = rim_in.at[p, 0 if dx < 0 else 1]
                spot[...] = jnp.zeros(spot.shape, BF)

    def regroup(p):
        for dx in (-1, 1):
            @pl.when(has_x[dx])
            def _(dx=dx):
                rim_arrival(p, dx).wait_recv()
        count = counts[p]
        own = quot[p, :, :count, :].reshape(ny * count, nx).astype(BF)
        rim = jnp.concatenate(
            [
                jnp.concatenate([rim_in[p, q, g, :count, :] for q in range(2)], axis=1)
                for g in range(lots)
            ],
            axis=0,
        )
        result = passes_xy(own, rim, too.at[1], wide.at[1], ky.at[1], ny, count, nx)
        for k in range(count // PAD):
            pair = [
                result[:, i * nx : (i + 1) * nx].reshape(ny, 8, nx) for i in (2 * k, 2 * k + 1)
            ]
            leaving[p, :, k * PAD : (k + 1) * PAD, :] = jnp.concatenate(pair, axis=1).astype(BF)
        for d in range(1, ngz):
            exchange(d, p).start()
        gathered[p, gz, :, :count, :] = leaving[p, pl.ds(gz * planes, planes), :count, :]

    load_est.wait()
    ext[:, PAD : PAD + nz, :] = est_ref[...].astype(BF)
    pl.semaphore_wait(barrier, total)
    send(0, above)
    pack_edges(lambda y: est_ref[y], packed, ny, nz, nx)
    send(0, corners + sideways)
    view = view_ref[0]
    for flip in range(2):
        make_matrices(
            taps_ref, view, extents_ref, bool(flip),
            mz_all if flip else mz, too.at[flip], wide.at[flip], ky.at[flip], ny, nz, nx,
        )
    clear(0)
    load_mea.wait()
    receive(0, sideways)
    quotients(0)
    for d in range(1, ngz):
        exchange(d, 2).start()
    make_table(table_ref, nz * ngz)
    est_lines[:, pl.ds(pl.multiple_of(gz * nz, nz), nz), :] = ext[
        pl.ds(gz * planes, planes), PAD : PAD + nz, :
    ]
    regroup(0)
    receive(0, above + corners)
    quotients(1)
    regroup(1)
    for d in range(1, ngz):
        for p in (2, 0, 1):
            exchange(d, p).wait_recv()
    lines = []
    for y in range(planes):
        line = []
        for g in range(ngz):
            line += [
                gathered[1, g, y, :PAD, :],
                gathered[0, g, y, : counts[0], :],
                gathered[1, g, y, PAD : 2 * PAD, :],
            ]
        lines.append(jnp.concatenate(line, axis=0))
    correction = dot(mz_all[...], jnp.concatenate(lines, axis=1))
    estimate = jnp.concatenate([est_lines[y] for y in range(planes)], axis=1)
    rounded = (estimate.astype(F32) * correction).astype(BF)
    step = nz * ngz
    for b in range(UP):
        rows = slice(b * step, (b + 1) * step)
        whole = dot(table_ref[rows, :], rounded)
        for y in range(planes):
            out_ref[y, rows, :] = whole[:, y * nx : (y + 1) * nx]
    sent(0)
    for p in range(2):
        for dx in (-1, 1):
            @pl.when(has_x[dx])
            def _(p=p, dx=dx):
                rim_copy(p, dx).wait_send()
    for d in range(1, ngz):
        for p in range(3):
            exchange(d, p).wait_send()


def on_device(ngx, ngz, view_index, psf_taps, extents, estimate, measured):
    ny, nz, nx = estimate.shape
    planes, lines = ny // ngz, nz * ngz
    group = nx // PAD
    half = max(2 * PAD, nz - 2 * PAD)
    smem = pl.BlockSpec(memory_space=pltpu.SMEM)
    vmem = pl.BlockSpec(memory_space=pltpu.VMEM)
    anywhere = pl.BlockSpec(memory_space=pl.ANY)
    return pl.pallas_call(
        functools.partial(kernel, ngx, ngz),
        out_shape=pltpu.VMEM((planes, UP * lines, nx), F32),
        in_specs=[smem, smem, smem, anywhere, anywhere],
        out_specs=vmem,
        scratch_shapes=[
            pltpu.VMEM((ny, nz, nx), F32),
            pltpu.VMEM((ny, nz, nx), F32),
            pltpu.VMEM((UP * lines, lines), BF),
            pltpu.VMEM((ny, nz + 2 * PAD, nx), BF),
            pltpu.VMEM((2, ny // group, nz + 2 * PAD, nx), BF),
            pltpu.VMEM((2, ny // group, nz, nx), BF),
            pltpu.VMEM((2, ny, half, nx), F32),
            pltpu.VMEM((2, 2, ny // group, half, nx), BF),
            pltpu.VMEM((2, 2, ny // group, half, nx), BF),
            pltpu.VMEM((2, ny, half, nx), BF),
            pltpu.VMEM((2, ngz, planes, half, nx), BF),
            pltpu.VMEM((planes, lines, nx), BF),
            pltpu.VMEM((nz, nz + 2 * PAD), BF),
            pltpu.VMEM((lines, lines), BF),
            pltpu.VMEM((2, nx, nx), BF),
            pltpu.VMEM((2, 2 * nx, group * nx), BF),
            pltpu.VMEM((2, ny * 8, ny * 8), BF),
            pltpu.SemaphoreType.DMA((8,)),
            pltpu.SemaphoreType.DMA((8,)),
            pltpu.SemaphoreType.DMA((2, 2)),
            pltpu.SemaphoreType.DMA((2, 2)),
            pltpu.SemaphoreType.DMA((ngz, 3)),
            pltpu.SemaphoreType.DMA((ngz, 3)),
            pltpu.SemaphoreType.DMA((2,)),
        ],
        compiler_params=pltpu.CompilerParams(collective_id=0, has_side_effects=True),
    )(view_index, psf_taps, extents.T, estimate, measured)


def solution(mesh):
    return jax.shard_map(
        functools.partial(on_device, mesh.shape["gx"], mesh.shape["gz"]),
        mesh=mesh,
        in_specs=(P(), P(), P(), P(None, "gz", "gx"), P(None, "gz", "gx")),
        out_specs=P("gz", None, "gx"),
        check_vma=False,
    )
```
